32 devices in a mesh: batch: 8 (over z, core), seq: 4 (over y, x).
Axes of the slice: x: 2, y: 2, z: 4, core: 2. Of those that a mesh axis runs over, the one named last changes fastest.
Arguments:
- token_cond: bfloat16 [16384, 768], P(('batch', 'seq')), parts along dimension 0, may hold values from -6 to 6
- atom_feat: bfloat16 [131072, 128], P(('batch', 'seq')), parts along dimension 0, may hold values from -16 to 16
- atom_counts: int32 [16384], P(('batch', 'seq')), parts along dimension 0, may hold values from 1 to 24, as said below
- w_token: bfloat16 [768, 128], replicated, may hold values from -0.21875 to 0.21875
- w_query: bfloat16 [128, 128], replicated, may hold values from -0.5 to 0.5
- w_key: bfloat16 [128, 128], replicated, may hold values from -0.5 to 0.5
- w_value: bfloat16 [128, 128], replicated, may hold values from -0.5 to 0.5
- w_out: bfloat16 [128, 128], replicated, may hold values from -0.5 to 0.5
- w_back: bfloat16 [128, 768], replicated, may hold values from -0.5 to 0.5
Outputs:
- token_out: bfloat16 [16384, 768], P(('batch', 'seq')), parts along dimension 0
- atom_out: bfloat16 [131072, 128], P(('batch', 'seq')), parts along dimension 0
The draws below stay inside these ranges and needn't reach their ends.
There are 8 independent parts, one for each index of `batch`. The reference program is written for one: setup_inputs(seed, part) draws one part's arguments, and reference() takes and returns one part's arrays. A program takes and returns all parts, laid end to end along the dimension named above; an argument that names none is the same for every part. Nothing has to cross between parts.
Inputs may be any that keep to these rules, and one draw needn't show every extreme that they name: `atom_counts`: every token has at least one atom and the counts of one complex sum to 16384. For every k, the atoms k * 4096 to (k + 1) * 4096 - 1 belong to tokens of (k - 1) * 512 to (k + 2) * 512 - 1.
All inputs are finite; a program needn't handle non-finite values.
Results may differ from the reference program's by a relative error of at most 0.0095.
The reference program's roundings to bfloat16 on the way count: a program that leaves them out, or rounds other values in their place, can miss the bound.
Values may be sent and summed in bfloat16 or wider, within the bound.
A program may use at most 128 MiB of HBM per device.

```python
import jax
import jax.numpy as jnp

CT = 768
CA = 128
HEADS = 4
HEAD = 32
QBLOCK = 32
KEYS = 128
MOST = 24
TOK_DEV = 512
ATOM_DEV = 4096
HALO = 48
NTOK = 2048
NATOM = 16384


def draw_atom_feat(key, part):
    first = jax.random.fold_in(jax.random.fold_in(key, 11), 0)
    values = jax.random.normal(first, (NATOM, CA), jnp.float32)
    values = jnp.clip(values, -6.0, 6.0)
    return values.astype(jnp.bfloat16)


def draw_atom_counts(key, part):
    first, second, third, fourth, fifth = jax.random.split(jax.random.fold_in(key, 23), 5)
    nblocks = NTOK // TOK_DEV
    slots = MOST - 1
    magnitude = jax.random.randint(first, (nblocks - 1,), 2 * TOK_DEV, 3 * TOK_DEV + 1)
    flip = jax.random.randint(second, (), 0, 2)
    signs = 1 - 2 * ((jnp.arange(nblocks - 1, dtype=jnp.int32) + flip) % 2)
    drift = jnp.concatenate([jnp.zeros((1,), jnp.int32), (magnitude * signs).astype(jnp.int32), jnp.zeros((1,), jnp.int32)])
    block_sum = ATOM_DEV + drift[1:] - drift[:-1]
    extra = block_sum - TOK_DEV
    levels = jax.random.randint(third, (nblocks, TOK_DEV // 4), 0, 4)
    token_level = jnp.repeat(levels, 4, axis=1)
    widest = jnp.argmax(extra).astype(jnp.int32)
    chosen_token = jax.random.randint(fourth, (), 0, TOK_DEV)
    forced = (jnp.arange(nblocks, dtype=jnp.int32)[:, None] == widest) & (jnp.arange(TOK_DEV, dtype=jnp.int32)[None, :] == chosen_token)
    token_level = jnp.where(forced, 4, token_level)
    noise = jax.random.randint(fifth, (nblocks, TOK_DEV, slots), 0, 4096)
    score = (token_level[:, :, None] * 4096 + noise).reshape(nblocks, TOK_DEV * slots)
    order = jnp.argsort(-score, axis=1, stable=True)
    rank = jnp.argsort(order, axis=1, stable=True)
    taken = (rank < extra[:, None]).astype(jnp.int32)
    counts = 1 + jnp.sum(taken.reshape(nblocks, TOK_DEV, slots), axis=2)
    return counts.reshape(NTOK).astype(jnp.int32)


def shard_levels(rng, dims, shards, low, top_value):
    gain = 1.0
    for dim, parts in shards:
        draws = jax.random.uniform(jax.random.fold_in(jax.random.fold_in(rng, 6), dim), (parts,), jnp.float32, low / len(shards), top_value / len(shards))
        gain = gain * jnp.repeat(jnp.exp(draws), dims[dim] // parts).reshape((-1,) + (1,) * (len(dims) - 1 - dim))
    return gain


def gaussian(rng, extent, width, limit, cuts=(), kind=jnp.bfloat16):
    drawn = width * jax.random.normal(rng, extent, jnp.float32)
    if cuts:
        drawn = drawn * shard_levels(rng, extent, cuts, -0.22, 0.18)
    return jnp.clip(drawn, -limit, limit).astype(kind)


def setup_inputs(seed: int = 0, part: int = 0) -> dict:
    splits = jax.random.split(jax.random.key(seed), 10)
    own_keys = jax.random.split(jax.random.fold_in(splits[9], part), 10)
    return {
        "token_cond": gaussian(own_keys[0], (NTOK, CT), 1.0, 6.0, ((0, 4),)),
        "atom_feat": draw_atom_feat(jax.random.fold_in(jax.random.fold_in(splits[9], part), 71), part),
        "atom_counts": draw_atom_counts(jax.random.fold_in(jax.random.fold_in(splits[9], part), 71), part),
        "w_token": gaussian(splits[3], (CT, CA), CT ** -0.5, 0.21875),
        "w_query": gaussian(splits[4], (CA, CA), CA ** -0.5, 0.5),
        "w_key": gaussian(splits[5], (CA, CA), CA ** -0.5, 0.5),
        "w_value": gaussian(splits[6], (CA, CA), CA ** -0.5, 0.5),
        "w_out": gaussian(splits[7], (CA, CA), CA ** -0.5, 0.5),
        "w_back": gaussian(splits[8], (CA, CT), CA ** -0.5, 0.5),
    }


def reference(token_cond, atom_feat, atom_counts, w_token, w_query, w_key, w_value, w_out, w_back):
    proj = jnp.dot(token_cond, w_token, preferred_element_type=jnp.float32).astype(jnp.bfloat16)
    ends = jnp.cumsum(atom_counts).astype(jnp.int32)
    atom_ids = jnp.arange(NATOM, dtype=jnp.int32)
    owner = jnp.searchsorted(ends, atom_ids, side='right').astype(jnp.int32)
    x = (atom_feat.astype(jnp.float32) + proj[owner].astype(jnp.float32)).astype(jnp.bfloat16)
    query = jnp.dot(x, w_query, preferred_element_type=jnp.float32).astype(jnp.bfloat16)
    keyed = jnp.dot(x, w_key, preferred_element_type=jnp.float32).astype(jnp.bfloat16)
    valued = jnp.dot(x, w_value, preferred_element_type=jnp.float32).astype(jnp.bfloat16)
    blocks = NATOM // QBLOCK
    span = KEYS // QBLOCK
    padk = jnp.pad(keyed, ((HALO, HALO), (0, 0))).reshape(blocks + span - 1, QBLOCK, HEADS, HEAD)
    padv = jnp.pad(valued, ((HALO, HALO), (0, 0))).reshape(blocks + span - 1, QBLOCK, HEADS, HEAD)
    keys = jnp.concatenate([padk[j:j + blocks] for j in range(span)], axis=1)
    values = jnp.concatenate([padv[j:j + blocks] for j in range(span)], axis=1)
    qblocks = query.reshape(blocks, QBLOCK, HEADS, HEAD)
    scores = jnp.einsum('bqhd,bkhd->bhqk', qblocks.astype(jnp.float32), keys.astype(jnp.float32)) / jnp.sqrt(jnp.float32(HEAD))
    key_pos = jnp.arange(blocks, dtype=jnp.int32)[:, None] * QBLOCK + jnp.arange(KEYS, dtype=jnp.int32)[None, :] - HALO
    valid = (key_pos >= 0) & (key_pos < NATOM)
    scores = jnp.where(valid[:, None, None, :], scores, jnp.float32(-1e+30))
    weights = jax.nn.softmax(scores, axis=-1).astype(jnp.bfloat16)
    attended = jnp.einsum('bhqk,bkhd->bqhd', weights.astype(jnp.float32), values.astype(jnp.float32))
    attended = attended.reshape(NATOM, CA).astype(jnp.bfloat16)
    atom_out = (x.astype(jnp.float32) + jnp.dot(attended, w_out, preferred_element_type=jnp.float32)).astype(jnp.bfloat16)
    sums = jax.ops.segment_sum(atom_out.astype(jnp.float32), owner, num_segments=NTOK)
    pooled = (sums / atom_counts.astype(jnp.float32)[:, None]).astype(jnp.bfloat16)
    token_out = (token_cond.astype(jnp.float32) + jnp.dot(pooled, w_back, preferred_element_type=jnp.float32)).astype(jnp.bfloat16)
    return (token_out, atom_out)
```

```python
import functools
import math

import jax
import jax.numpy as jnp
from jax import lax
from jax.experimental import pallas as pl
from jax.experimental.pallas import tpu as pltpu
from jax.sharding import PartitionSpec as P

HEADS = 4
QBLOCK = 32
KEYS = 128
HALO = 48
LANES = 128
MESH = pl.DeviceIdType.MESH
F32 = jnp.float32
BF16 = jnp.bfloat16


def dot(a, b, dims=((1,), (0,))):
    return lax.dot_general(a, b, (dims, ((), ())), preferred_element_type=F32)


def greet(n, me):
    barrier = pltpu.get_barrier_semaphore()
    for d in range(1, n):
        pl.semaphore_signal(barrier, inc=1, device_id={"seq": lax.rem(me + d, n)}, device_id_type=MESH)
    return lambda: pl.semaphore_wait(barrier, n - 1)


def whole(n, group, cond_h, wtok_h, feat_h, counts_h, wq_h, wk_h, wv_h, wout_h, obuf, pooled_ref,
          cond, wtok, feat, wqkv, wout, table, halo, cnt, padded, ends_all, ends_v, starts_v, wins_v, wins, cols,
          xs, qs, ks, vs, att, mem, hmem, run, sbuf, got, lsem, csend, crecv, send_sem, recv_sem, ssend, srecv):
    me = lax.axis_index("seq")
    tok = cond.shape[0]
    atom_rows, width = feat.shape
    crow = tok // LANES
    head = width // HEADS
    nrow = ends_v.shape[0]
    scale = math.log2(math.e) / math.sqrt(head)
    step = group * LANES
    tiles = atom_rows // LANES
    groups = atom_rows // step
    right, left = lax.rem(me + 1, n), lax.rem(me + n - 1, n)
    right2, left2 = lax.rem(me + 2, n), lax.rem(me + n - 2, n)

    arrive = greet(n, me)
    loads = [pltpu.make_async_copy(counts_h, cnt.at[me], lsem.at[0]),
             pltpu.make_async_copy(wtok_h, wtok, lsem.at[1])]
    loads += [pltpu.make_async_copy(cond_h.at[pl.ds(r * LANES, LANES)], cond.at[pl.ds(r * LANES, LANES)],
                                    lsem.at[8 + r]) for r in range(crow)]
    loads.append(pltpu.make_async_copy(feat_h, feat, lsem.at[2]))
    loads += [pltpu.make_async_copy(w, wqkv.at[:, pl.ds(i * width, width)], lsem.at[3 + i])
              for i, w in enumerate((wq_h, wk_h, wv_h))]
    loads.append(pltpu.make_async_copy(wout_h, wout, lsem.at[6]))
    for c in loads:
        c.start()

    base = LANES + tok
    table[pl.ds(0, LANES - HALO), :] = jnp.zeros((LANES - HALO, width), BF16)
    table[pl.ds(LANES + 3 * tok + HALO, 2 * LANES - HALO), :] = jnp.zeros((2 * LANES - HALO, width), BF16)
    run[pl.ds(0, 2 * LANES), :] = jnp.zeros((2 * LANES, width), F32)
    padded[...] = jnp.zeros_like(padded)
    loads[1].wait()
    for r in range(crow):
        loads[2 + r].wait()
        table[pl.ds(base + r * LANES, LANES), :] = dot(cond[pl.ds(r * LANES, LANES), :], wtok[...]).astype(BF16)
    loads[0].wait()
    loads[2 + crow].wait()
    arrive()

    ccopies = [pltpu.make_async_remote_copy(
        src_ref=cnt.at[me], dst_ref=cnt.at[me], send_sem=csend.at[d - 1], recv_sem=crecv.at[d - 1],
        device_id={"seq": lax.rem(me + d, n)}, device_id_type=MESH) for d in range(1, n)]

    def remote(i, src, dst, dev):
        return pltpu.make_async_remote_copy(
            src_ref=src, dst_ref=dst, send_sem=send_sem.at[i], recv_sem=recv_sem.at[i],
            device_id={"seq": dev}, device_id_type=MESH)

    copies = [
        remote(0, feat.at[pl.ds(atom_rows - HALO, HALO)], halo.at[pl.ds(0, HALO)], right),
        remote(1, feat.at[pl.ds(0, HALO)], halo.at[pl.ds(HALO, HALO)], left),
        remote(2, table.at[pl.ds(base + tok - HALO, HALO)], table.at[pl.ds(LANES - HALO, HALO)], right2),
        remote(3, table.at[pl.ds(base, HALO)], table.at[pl.ds(LANES + 3 * tok, HALO)], left2),
        remote(4, table.at[pl.ds(base, tok)], table.at[pl.ds(LANES, tok)], right),
        remote(5, table.at[pl.ds(base, tok)], table.at[pl.ds(LANES + 2 * tok, tok)], left),
    ]
    for c in ccopies + copies:
        c.start()

    def column(r):
        return jnp.transpose(jnp.broadcast_to(cnt[me, pl.ds(r, 1), :].astype(F32), (LANES, LANES)))

    for r in range(crow):
        cols[pl.ds(r * LANES, LANES), :] = column(r)
    for c in ccopies:
        c.wait()
    rows = padded.shape[0]
    for j in range(n):
        padded[pl.ds(8 + crow * j, crow), :] = cnt[j]
    counts = padded[...].astype(F32).astype(BF16)
    tri = (lax.broadcasted_iota(jnp.int32, (LANES, LANES), 0)
           <= lax.broadcasted_iota(jnp.int32, (LANES, LANES), 1)).astype(F32).astype(BF16)
    before = (lax.broadcasted_iota(jnp.int32, (rows, rows), 1)
              < lax.broadcasted_iota(jnp.int32, (rows, rows), 0)).astype(F32).astype(BF16)
    inner = dot(counts, tri)
    outer = jnp.sum(dot(before, counts), axis=1, keepdims=True)
    ends_all[...] = (inner + outer).astype(jnp.int32)
    near = pl.ds(8 - 1 - crow + crow * me, nrow)
    ends = ends_all[near, :] - me * atom_rows
    ends_v[...] = ends
    starts_v[...] = ends - padded[near, :]
    sizes = jnp.sum(padded[...], axis=1, keepdims=True)
    start = 8 - 1 - crow + crow * me
    past = lax.broadcasted_iota(jnp.int32, (rows, 1), 0) < start
    mark = jnp.sum(jnp.where(past, sizes, 0), axis=0, keepdims=True) - me * atom_rows
    near_sizes = jnp.sum(padded[near, :], axis=1, keepdims=True)
    first = jnp.where(lax.broadcasted_iota(jnp.int32, (8, LANES), 0) == 0,
                      lax.broadcasted_iota(jnp.int32, (8, LANES), 1) * LANES, -HALO)
    w = jnp.zeros_like(first)
    for r in range(nrow - 1):
        mark = mark + near_sizes[r:r + 1, :]
        w += jnp.where(mark <= first, 1, 0)
    w = jnp.minimum(w, nrow - 3)
    wins_v[pl.ds(0, 8), :] = w
    held = lax.broadcasted_iota(jnp.int32, (1, LANES), 1) < tiles
    w0 = jnp.where(held, w[0:1, :], nrow)
    block = lax.broadcasted_iota(jnp.int32, (nrow, LANES), 0)
    seen = jnp.sum(jnp.where(w0 <= block, 1, 0), axis=1, keepdims=True)
    last = w[0:1, tiles - 1:tiles]
    wins_v[pl.ds(8, nrow), :] = jnp.where(
        block <= last, seen * 2, jnp.where(block == last + 1, 2 * tiles + 1, 0))
    down = pltpu.make_async_copy(wins_v, wins, lsem.at[7])
    down.start()
    down.wait()

    def each(f):
        def body(g, c):
            f(g)
            return c
        return body

    def members(w, first, r):
        ids = first + lax.broadcasted_iota(jnp.int32, (r, LANES), 0)
        parts = []
        for s in range(2):
            lo = starts_v[pl.ds(w + s, 1), :]
            hi = ends_v[pl.ds(w + s, 1), :]
            parts.append(jnp.where((ids >= lo) & (ids < hi), F32(1), F32(0)).astype(BF16))
        return jnp.concatenate(parts, axis=1)

    def gather(w, member, f):
        picked = dot(member, table[pl.ds(w * LANES, 2 * LANES), :])
        return (f.astype(F32) + picked).astype(BF16)

    def build(i):
        a = pl.multiple_of(i * LANES, LANES)
        mem[pl.ds(a, LANES), :] = members(wins[0, i], a, LANES)

    lax.fori_loop(0, tiles, each(build), 0)
    outside = ((-HALO, 0, wins[1, 0]), (atom_rows, atom_rows + HALO, wins[0, tiles]))
    for i, (start, _, w) in enumerate(outside):
        hmem[pl.ds(i * HALO, HALO), :] = members(w, jnp.int32(start), HALO)
    for c in loads[3 + crow:]:
        c.wait()
    for c in copies:
        c.wait()

    def keyval(at, qkv, r):
        ks[pl.ds(at, r), :] = qkv[:, width:2 * width].astype(BF16)
        vs[pl.ds(at, r), :] = qkv[:, 2 * width:].astype(BF16)

    for i, (_, at, w) in enumerate(outside):
        x = gather(w, hmem[pl.ds(i * HALO, HALO), :], halo[pl.ds(i * HALO, HALO), :])
        keyval(at, dot(x, wqkv[...]), HALO)

    lane = lax.broadcasted_iota(jnp.int32, (1, width), 1)
    hmask = [((lane >= h * head) & (lane < (h + 1) * head)) for h in range(HEADS)]
    hmul = [jnp.where(m, F32(1), F32(0)).astype(BF16) for m in hmask]
    ones = jnp.ones((KEYS, width), BF16)
    total = atom_rows * n
    klane = lax.broadcasted_iota(jnp.int32, (1, KEYS), 1)
    per = LANES // QBLOCK

    def pick(o):
        r = o[(HEADS - 1) * QBLOCK:]
        for h in range(HEADS - 2, -1, -1):
            r = jnp.where(hmask[h], o[h * QBLOCK:(h + 1) * QBLOCK], r)
        return r

    def gathers(g):
        made = []
        for u in range(group):
            a = pl.multiple_of(g * step + u * LANES, LANES)
            made.append((a, gather(wins[0, g * group + u], mem[pl.ds(a, LANES), :], feat[pl.ds(a, LANES), :])))
        return made

    def project(made):
        qkvs = [dot(x, wqkv[...]) for _, x in made]
        for (a, x), qkv in zip(made, qkvs):
            xs[pl.ds(a, LANES), :] = x
            qs[pl.ds(a, LANES), :] = qkv[:, :width].astype(BF16)
            keyval(pl.multiple_of(a + HALO, 16), qkv, LANES)

    def scored(g, js):
        scores = []
        for j in js:
            at = pl.multiple_of(g * step + j * QBLOCK, QBLOCK)
            q = qs[pl.ds(at, QBLOCK), :]
            qb = jnp.concatenate([q * m for m in hmul], axis=0)
            s = dot(qb, ks[pl.ds(at, KEYS), :], ((1,), (1,)))
            pos = me * atom_rows + at - HALO + klane
            scores.append(jnp.where((pos >= 0) & (pos < total), s, F32(-1e30)))
        return scores

    def soft(scores):
        probs = []
        for s in scores:
            m = jnp.max(s, axis=1, keepdims=True)
            probs.append(jnp.exp2((s - m) * F32(scale)).astype(BF16))
        return probs

    def attend(g, js, probs):
        raw = []
        for j, p in zip(js, probs):
            at = pl.multiple_of(g * step + j * QBLOCK, QBLOCK)
            raw.append(dot(p, jnp.concatenate([vs[pl.ds(at, KEYS), :], ones], axis=1)))
        return [(pick(o[:, :width]) / pick(o[:, width:])).astype(BF16) for o in raw]

    def residual(g):
        at = pl.ds(pl.multiple_of(g * step, step), step)
        y = (xs[at, :].astype(F32) + dot(att[at, :], wout[...])).astype(BF16)
        obuf[at, :] = y
        return y

    def pooled(g, y):
        parts = [dot(mem[pl.ds(pl.multiple_of(g * step + u * LANES, LANES), LANES), :],
                     y[u * LANES:(u + 1) * LANES], ((0,), (0,))) for u in range(group)]
        at = pl.multiple_of(2 * step * g, 2 * step)
        acc = run[pl.ds(at, 2 * LANES), :]
        for u, part in enumerate(parts):
            i = g * group + u
            same = wins[0, i] == wins[0, jnp.maximum(i - 1, 0)]
            low = jnp.where(same, acc[:LANES], acc[LANES:])
            high = jnp.where(same, acc[LANES:], F32(0))
            acc = part + jnp.concatenate([low, high], axis=0)
            run[pl.ds(pl.multiple_of(at + (u + 1) * 2 * LANES, 2 * LANES), 2 * LANES), :] = acc

    early, late = range(group * per // 2), range(group * per // 2, group * per)
    ahead = 2

    def advance(g, more):
        past = jnp.maximum(g - 1, 0)
        s0 = scored(g, early)
        y = residual(past)
        made = gathers(g + ahead) if more else None
        p0 = soft(s0)
        s1 = scored(g, late)
        pooled(past, y)
        o0 = attend(g, early, p0)
        p1 = soft(s1)
        o1 = attend(g, late, p1)
        if more:
            project(made)
        att[pl.ds(pl.multiple_of(g * step, step), step), :] = jnp.concatenate(o0 + o1, axis=0)

    lax.fori_loop(0, ahead, each(lambda g: project(gathers(g))), 0)
    lax.fori_loop(0, groups - ahead, each(lambda g: advance(g, True)), 0)
    lax.fori_loop(groups - ahead, groups, each(lambda g: advance(g, False)), 0)
    y = residual(groups - 1)
    pooled(groups - 1, y)

    def sums(b):
        return run[pl.ds(wins[8 + b, 0] * LANES, LANES), :]

    sides = []
    for r in range(crow):
        for i, (b, dev) in enumerate(((1 + r, left), (1 + 2 * crow + r, right))):
            at = pl.ds(r * LANES, LANES)
            sbuf[i, at, :] = sums(b).astype(BF16)
            c = pltpu.make_async_remote_copy(
                src_ref=sbuf.at[i, at], dst_ref=got.at[i, at], send_sem=ssend.at[i, r], recv_sem=srecv.at[i, r],
                device_id={"seq": dev}, device_id_type=MESH)
            c.start()
            sides.append(c)
    for r in range(crow):
        for c in sides[2 * r:2 * r + 2]:
            c.wait()
        at = pl.ds(r * LANES, LANES)
        s = sums(1 + crow + r) + got[0, at, :].astype(F32) + got[1, at, :].astype(F32)
        pooled_ref[at, :] = (s / cols[at, :]).astype(BF16)


def finish(atoms_ref, pooled_ref, cond_ref, wback_ref, token_ref, out_ref, tbuf, sem):
    tok = cond_ref.shape[0]
    out = pltpu.make_async_copy(atoms_ref, out_ref, sem.at[0])
    out.start()
    copies = []
    for r in range(tok // LANES):
        at = pl.ds(r * LANES, LANES)
        tbuf[at, :] = (cond_ref[at, :].astype(F32) + dot(pooled_ref[at, :], wback_ref[...])).astype(BF16)
        c = pltpu.make_async_copy(tbuf.at[at], token_ref.at[at], sem.at[1 + r])
        c.start()
        copies.append(c)
    for c in copies:
        c.wait()
    out.wait()


VM = pl.BlockSpec(memory_space=pltpu.VMEM)
ANY = pl.BlockSpec(memory_space=pl.ANY)
HBM = pl.BlockSpec(memory_space=pltpu.HBM)


def shards(n, token_cond, atom_feat, atom_counts, w_token, w_query, w_key, w_value, w_out, w_back):
    tok, ct = token_cond.shape
    atom_rows, width = atom_feat.shape
    crow = tok // LANES
    counts = atom_counts.reshape(crow, LANES)
    nrow = 3 * crow + 4
    trows = 3 * tok + 3 * LANES
    tiles = atom_rows // LANES
    S = jax.ShapeDtypeStruct
    V = pltpu.VMEM
    DMA = pltpu.SemaphoreType.DMA
    prows = -(-(8 + crow * n + nrow) // 8) * 8
    group = 2
    I32 = jnp.int32
    hold = lambda x: pltpu.with_memory_space_constraint(x, pltpu.HBM)
    atoms, pooled = pl.pallas_call(
        functools.partial(whole, n, group),
        name="whole",
        out_shape=(S((atom_rows, width), BF16), S((tok, width), BF16)),
        in_specs=[HBM] * 8,
        out_specs=(VM, VM),
        scratch_shapes=[
            V((tok, ct), BF16), V((ct, width), BF16), V((atom_rows, width), BF16), V((width, 3 * width), BF16),
            V((width, width), BF16), V((trows, width), BF16), V((2 * HALO, width), BF16),
            V((n, crow, LANES), I32), V((prows, LANES), I32), V((prows, LANES), I32),
            V((nrow, LANES), I32), V((nrow, LANES), I32), V((8 + nrow, LANES), I32),
            pltpu.SMEM((8 + nrow, LANES), I32), V((tok, LANES), F32),
            V((atom_rows, width), BF16), V((atom_rows, width), BF16),
            V((atom_rows + 2 * HALO, width), BF16), V((atom_rows + 2 * HALO, width), BF16),
            V((atom_rows, width), BF16), V((atom_rows, 2 * LANES), BF16), V((2 * HALO, 2 * LANES), BF16),
            V(((tiles + 1) * 2 * LANES, width), F32),
            V((2, tok, width), BF16), V((2, tok, width), BF16),
            DMA((8 + crow,)), DMA((n - 1,)), DMA((n - 1,)), DMA((6,)), DMA((6,)), DMA((2, crow)), DMA((2, crow)),
        ],
        compiler_params=pltpu.CompilerParams(collective_id=0, has_side_effects=True, vmem_limit_bytes=24 << 20),
    )(*[hold(x) for x in (token_cond, w_token, atom_feat, counts, w_query, w_key, w_value, w_out)])
    token_out, atom_out = pl.pallas_call(
        finish,
        name="finish",
        out_shape=(S((tok, ct), BF16), S((atom_rows, width), BF16)),
        in_specs=[VM, VM, VM, VM],
        out_specs=(ANY, ANY),
        scratch_shapes=[V((tok, ct), BF16), DMA((1 + crow,))],
        compiler_params=pltpu.CompilerParams(vmem_limit_bytes=8 << 20),
    )(atoms, pooled, token_cond, w_back)
    return (token_out, atom_out)


def solution(mesh):
    both = P(("batch", "seq"), None)
    in_specs = (both, both, P(("batch", "seq")), P(), P(), P(), P(), P(), P())
    return jax.shard_map(
        functools.partial(shards, mesh.shape["seq"]), mesh=mesh, in_specs=in_specs, out_specs=(both, both),
        check_vma=False)
```

```python
import functools
import math

import jax
import jax.numpy as jnp
from jax import lax
from jax.experimental import pallas as pl
from jax.experimental.pallas import tpu as pltpu
from jax.sharding import PartitionSpec as P

HEADS = 4
QBLOCK = 32
KEYS = 128
HALO = 48
LANES = 128
MOST = 24
MESH = pl.DeviceIdType.MESH
F32 = jnp.float32
BF16 = jnp.bfloat16


def dot(a, b, dims=((1,), (0,))):
    return lax.dot_general(a, b, (dims, ((), ())), preferred_element_type=F32)


def greet(n, me):
    barrier = pltpu.get_barrier_semaphore()
    for d in range(1, n):
        pl.semaphore_signal(barrier, inc=1, device_id={"seq": lax.rem(me + d, n)}, device_id_type=MESH)
    return lambda: pl.semaphore_wait(barrier, n - 1)


def whole(n, group, cond_h, wtok_h, feat_h, counts_h, wq_h, wk_h, wv_h, wout_h, obuf, pooled_ref,
          cond, wtok, feat, wqkv, wout, table, halo, cnt, padded, ends_all, ends_v, starts_v, wins_v, wins, cols,
          xs, qs, ks, vs, att, mem, hmem, run, sbuf, got, lsem, csend, crecv, send_sem, recv_sem, ssend, srecv):
    me = lax.axis_index("seq")
    tok = cond.shape[0]
    atom_rows, width = feat.shape
    crow = tok // LANES
    head = width // HEADS
    nrow = ends_v.shape[0]
    scale = math.log2(math.e) / math.sqrt(head)
    step = group * LANES
    tiles = atom_rows // LANES
    groups = atom_rows // step
    right, left = lax.rem(me + 1, n), lax.rem(me + n - 1, n)
    right2, left2 = lax.rem(me + 2, n), lax.rem(me + n - 2, n)

    odd = lax.rem(me, 2)
    has_left, has_right = me > 0, me < n - 1

    def blank(at):
        table[pl.ds(at, tok), :] = jnp.zeros((tok, width), BF16)

    pl.when(me == 0)(lambda: blank(LANES))
    pl.when(me == n - 1)(lambda: blank(LANES + 2 * tok))
    arrive = greet(n, me)
    loads = [pltpu.make_async_copy(counts_h, cnt.at[me], lsem.at[0]),
             pltpu.make_async_copy(wtok_h, wtok, lsem.at[1])]
    loads += [pltpu.make_async_copy(cond_h.at[pl.ds(r * LANES, LANES)], cond.at[pl.ds(r * LANES, LANES)],
                                    lsem.at[8 + r]) for r in range(crow)]
    loads.append(pltpu.make_async_copy(feat_h, feat, lsem.at[2]))
    loads += [pltpu.make_async_copy(w, wqkv.at[:, pl.ds(i * width, width)], lsem.at[3 + i])
              for i, w in enumerate((wq_h, wk_h, wv_h))]
    loads.append(pltpu.make_async_copy(wout_h, wout, lsem.at[6]))
    for c in loads:
        c.start()

    base = LANES + tok
    table[pl.ds(0, LANES - HALO), :] = jnp.zeros((LANES - HALO, width), BF16)
    table[pl.ds(LANES + 3 * tok + HALO, 2 * LANES - HALO), :] = jnp.zeros((2 * LANES - HALO, width), BF16)
    run[pl.ds(0, 2 * LANES), :] = jnp.zeros((2 * LANES, width), F32)
    padded[...] = jnp.zeros_like(padded)
    loads[1].wait()
    for r in range(crow):
        loads[2 + r].wait()
        table[pl.ds(base + r * LANES, LANES), :] = dot(cond[pl.ds(r * LANES, LANES), :], wtok[...]).astype(BF16)
    loads[0].wait()
    loads[2 + crow].wait()
    arrive()

    ccopies = [pltpu.make_async_remote_copy(
        src_ref=cnt.at[me], dst_ref=cnt.at[me], send_sem=csend.at[d - 1], recv_sem=crecv.at[d - 1],
        device_id={"seq": lax.rem(me + d, n)}, device_id_type=MESH) for d in range(1, n)]

    def remote(i, src, dst, dev):
        return pltpu.make_async_remote_copy(
            src_ref=src, dst_ref=dst, send_sem=send_sem.at[i], recv_sem=recv_sem.at[i],
            device_id={"seq": dev}, device_id_type=MESH)

    copies = [
        remote(0, feat.at[pl.ds(atom_rows - HALO, HALO)], halo.at[pl.ds(0, HALO)], right),
        remote(1, feat.at[pl.ds(0, HALO)], halo.at[pl.ds(HALO, HALO)], left),
        remote(2, table.at[pl.ds(base + tok - HALO, HALO)], table.at[pl.ds(LANES - HALO, HALO)], right2),
        remote(3, table.at[pl.ds(base, HALO)], table.at[pl.ds(LANES + 3 * tok, HALO)], left2),
    ]
    for c in ccopies + copies:
        c.start()
    to_right = remote(4, table.at[pl.ds(base, tok)], table.at[pl.ds(LANES, tok)], right)
    to_left = remote(5, table.at[pl.ds(base, tok)], table.at[pl.ds(LANES + 2 * tok, tok)], left)
    pl.when((odd == 1) & has_right)(to_right.start)
    pl.when(has_left)(to_left.start)
    pl.when((odd == 0) & has_right)(to_right.start)

    def column(r):
        return jnp.transpose(jnp.broadcast_to(cnt[me, pl.ds(r, 1), :].astype(F32), (LANES, LANES)))

    for r in range(crow):
        cols[pl.ds(r * LANES, LANES), :] = column(r)
    for c in ccopies:
        c.wait()
    rows = padded.shape[0]
    for j in range(n):
        padded[pl.ds(8 + crow * j, crow), :] = cnt[j]
    counts = padded[...].astype(F32).astype(BF16)
    tri = (lax.broadcasted_iota(jnp.int32, (LANES, LANES), 0)
           <= lax.broadcasted_iota(jnp.int32, (LANES, LANES), 1)).astype(F32).astype(BF16)
    before = (lax.broadcasted_iota(jnp.int32, (rows, rows), 1)
              < lax.broadcasted_iota(jnp.int32, (rows, rows), 0)).astype(F32).astype(BF16)
    inner = dot(counts, tri)
    outer = jnp.sum(dot(before, counts), axis=1, keepdims=True)
    ends_all[...] = (inner + outer).astype(jnp.int32)
    near = pl.ds(8 - 1 - crow + crow * me, nrow)
    ends = ends_all[near, :] - me * atom_rows
    ends_v[...] = ends
    starts_v[...] = ends - padded[near, :]
    sizes = jnp.sum(padded[...], axis=1, keepdims=True)
    start = 8 - 1 - crow + crow * me
    past = lax.broadcasted_iota(jnp.int32, (rows, 1), 0) < start
    mark = jnp.sum(jnp.where(past, sizes, 0), axis=0, keepdims=True) - me * atom_rows
    near_sizes = jnp.sum(padded[near, :], axis=1, keepdims=True)
    first = jnp.where(lax.broadcasted_iota(jnp.int32, (8, LANES), 0) == 0,
                      lax.broadcasted_iota(jnp.int32, (8, LANES), 1) * LANES, -HALO)
    w = jnp.zeros_like(first)
    for r in range(nrow - 1):
        mark = mark + near_sizes[r:r + 1, :]
        w += jnp.where(mark <= first, 1, 0)
    w = jnp.minimum(w, nrow - 3)
    wins_v[pl.ds(0, 8), :] = w
    held = lax.broadcasted_iota(jnp.int32, (1, LANES), 1) < tiles
    w0 = jnp.where(held, w[0:1, :], nrow)
    block = lax.broadcasted_iota(jnp.int32, (nrow, LANES), 0)
    seen = jnp.sum(jnp.where(w0 <= block, 1, 0), axis=1, keepdims=True)
    last = w[0:1, tiles - 1:tiles]
    wins_v[pl.ds(8, nrow), :] = jnp.where(
        block <= last, seen * 2, jnp.where(block == last + 1, 2 * tiles + 1, 0))
    down = pltpu.make_async_copy(wins_v, wins, lsem.at[7])
    down.start()
    down.wait()

    def each(f):
        def body(g, c):
            f(g)
            return c
        return body

    def members(w, first, r):
        ids = first + lax.broadcasted_iota(jnp.int32, (r, LANES), 0)
        parts = []
        for s in range(2):
            lo = starts_v[pl.ds(w + s, 1), :]
            hi = ends_v[pl.ds(w + s, 1), :]
            parts.append(jnp.where((ids >= lo) & (ids < hi), F32(1), F32(0)).astype(BF16))
        return jnp.concatenate(parts, axis=1)

    def gather(w, member, f):
        picked = dot(member, table[pl.ds(w * LANES, 2 * LANES), :])
        return (f.astype(F32) + picked).astype(BF16)

    def build(i):
        a = pl.multiple_of(i * LANES, LANES)
        mem[pl.ds(a, LANES), :] = members(wins[0, i], a, LANES)

    lax.fori_loop(0, tiles, each(build), 0)
    outside = ((-HALO, 0, wins[1, 0]), (atom_rows, atom_rows + HALO, wins[0, tiles]))
    for i, (start, _, w) in enumerate(outside):
        hmem[pl.ds(i * HALO, HALO), :] = members(w, jnp.int32(start), HALO)
    for c in loads[3 + crow:]:
        c.wait()
    for c in copies:
        c.wait()
    pl.when(has_left)(to_right.wait_recv)
    pl.when(has_right)(to_left.wait_recv)

    def keyval(at, qkv, r):
        ks[pl.ds(at, r), :] = qkv[:, width:2 * width].astype(BF16)
        vs[pl.ds(at, r), :] = qkv[:, 2 * width:].astype(BF16)

    for i, (_, at, w) in enumerate(outside):
        x = gather(w, hmem[pl.ds(i * HALO, HALO), :], halo[pl.ds(i * HALO, HALO), :])
        keyval(at, dot(x, wqkv[...]), HALO)

    lane = lax.broadcasted_iota(jnp.int32, (1, width), 1)
    hmask = [((lane >= h * head) & (lane < (h + 1) * head)) for h in range(HEADS)]
    hmul = [jnp.where(m, F32(1), F32(0)).astype(BF16) for m in hmask]
    ones = jnp.ones((KEYS, width), BF16)
    total = atom_rows * n
    klane = lax.broadcasted_iota(jnp.int32, (1, KEYS), 1)
    per = LANES // QBLOCK

    def pick(o):
        r = o[(HEADS - 1) * QBLOCK:]
        for h in range(HEADS - 2, -1, -1):
            r = jnp.where(hmask[h], o[h * QBLOCK:(h + 1) * QBLOCK], r)
        return r

    def gathers(g):
        made = []
        for u in range(group):
            a = pl.multiple_of(g * step + u * LANES, LANES)
            made.append((a, gather(wins[0, g * group + u], mem[pl.ds(a, LANES), :], feat[pl.ds(a, LANES), :])))
        return made

    def project(made):
        qkvs = [dot(x, wqkv[...]) for _, x in made]
        for (a, x), qkv in zip(made, qkvs):
            xs[pl.ds(a, LANES), :] = x
            qs[pl.ds(a, LANES), :] = qkv[:, :width].astype(BF16)
            keyval(pl.multiple_of(a + HALO, 16), qkv, LANES)

    def scored(g, js):
        scores = []
        for j in js:
            at = pl.multiple_of(g * step + j * QBLOCK, QBLOCK)
            q = qs[pl.ds(at, QBLOCK), :]
            qb = jnp.concatenate([q * m for m in hmul], axis=0)
            s = dot(qb, ks[pl.ds(at, KEYS), :], ((1,), (1,)))
            pos = me * atom_rows + at - HALO + klane
            scores.append(jnp.where((pos >= 0) & (pos < total), s, F32(-1e30)))
        return scores

    def soft(scores):
        probs = []
        for s in scores:
            m = jnp.max(s, axis=1, keepdims=True)
            probs.append(jnp.exp2((s - m) * F32(scale)).astype(BF16))
        return probs

    def attend(g, js, probs):
        raw = []
        for j, p in zip(js, probs):
            at = pl.multiple_of(g * step + j * QBLOCK, QBLOCK)
            raw.append(dot(p, jnp.concatenate([vs[pl.ds(at, KEYS), :], ones], axis=1)))
        return [(pick(o[:, :width]) / pick(o[:, width:])).astype(BF16) for o in raw]

    def residual(g):
        at = pl.ds(pl.multiple_of(g * step, step), step)
        y = (xs[at, :].astype(F32) + dot(att[at, :], wout[...])).astype(BF16)
        obuf[at, :] = y
        return y

    def pooled(g, y):
        parts = [dot(mem[pl.ds(pl.multiple_of(g * step + u * LANES, LANES), LANES), :],
                     y[u * LANES:(u + 1) * LANES], ((0,), (0,))) for u in range(group)]
        at = pl.multiple_of(2 * step * g, 2 * step)
        acc = run[pl.ds(at, 2 * LANES), :]
        for u, part in enumerate(parts):
            i = g * group + u
            same = wins[0, i] == wins[0, jnp.maximum(i - 1, 0)]
            low = jnp.where(same, acc[:LANES], acc[LANES:])
            high = jnp.where(same, acc[LANES:], F32(0))
            acc = part + jnp.concatenate([low, high], axis=0)
            run[pl.ds(pl.multiple_of(at + (u + 1) * 2 * LANES, 2 * LANES), 2 * LANES), :] = acc

    def sums(b):
        return run[pl.ds(wins[8 + b, 0] * LANES, LANES), :]

    def side(i, dev, r):
        at = pl.ds(r * LANES, LANES)
        return pltpu.make_async_remote_copy(
            src_ref=sbuf.at[i, at], dst_ref=got.at[i, at], send_sem=ssend.at[i, r], recv_sem=srecv.at[i, r],
            device_id={"seq": dev}, device_id_type=MESH)

    def share(i, dev, r):
        sbuf[i, pl.ds(r * LANES, LANES), :] = sums(1 + 2 * crow * i + r).astype(BF16)
        side(i, dev, r).start()

    early, late = range(group * per // 2), range(group * per // 2, group * per)
    ahead = 1
    ready = min((groups - 1) * step // (MOST * LANES), crow) if ahead == 1 else 0


    def advance(g, more):
        past = jnp.maximum(g - 1, 0)
        s0 = scored(g, early)
        y = residual(past)
        made = gathers(g + ahead) if more else None
        p0 = soft(s0)
        if more:
            project(made)
        s1 = scored(g, late)
        pooled(past, y)
        if not more:
            for r in range(ready):
                pl.when(has_left)(functools.partial(share, 0, left, r))
        o0 = attend(g, early, p0)
        p1 = soft(s1)
        o1 = attend(g, late, p1)
        att[pl.ds(pl.multiple_of(g * step, step), step), :] = jnp.concatenate(o0 + o1, axis=0)

    lax.fori_loop(0, ahead, each(lambda g: project(gathers(g))), 0)
    lax.fori_loop(0, groups - ahead, each(lambda g: advance(g, True)), 0)
    lax.fori_loop(groups - ahead, groups, each(lambda g: advance(g, False)), 0)
    y = residual(groups - 1)
    pooled(groups - 1, y)

    for r in range(crow):
        pl.when((odd == 1) & has_right)(functools.partial(share, 1, right, r))
    for r in range(ready, crow):
        pl.when(has_left)(functools.partial(share, 0, left, r))
    for r in range(crow):
        pl.when((odd == 0) & has_right)(functools.partial(share, 1, right, r))
    for r in range(crow):
        at = pl.ds(r * LANES, LANES)
        pl.when(has_left)(side(1, right, r).wait_recv)
        pl.when(has_right)(side(0, left, r).wait_recv)
        s = (sums(1 + crow + r) + jnp.where(has_right, got[0, at, :].astype(F32), 0)
             + jnp.where(has_left, got[1, at, :].astype(F32), 0))
        pooled_ref[at, :] = (s / cols[at, :]).astype(BF16)
    pl.when(has_right)(to_right.wait_send)
    pl.when(has_left)(to_left.wait_send)
    for r in range(crow):
        pl.when(has_right)(side(1, right, r).wait_send)
        pl.when(has_left)(side(0, left, r).wait_send)


def finish(atoms_ref, pooled_ref, cond_ref, wback_ref, token_ref, out_ref, tbuf, sem):
    tok = cond_ref.shape[0]
    out = pltpu.make_async_copy(atoms_ref, out_ref, sem.at[0])
    out.start()
    copies = []
    for r in range(tok // LANES):
        at = pl.ds(r * LANES, LANES)
        tbuf[at, :] = (cond_ref[at, :].astype(F32) + dot(pooled_ref[at, :], wback_ref[...])).astype(BF16)
        c = pltpu.make_async_copy(tbuf.at[at], token_ref.at[at], sem.at[1 + r])
        c.start()
        copies.append(c)
    for c in copies:
        c.wait()
    out.wait()


VM = pl.BlockSpec(memory_space=pltpu.VMEM)
ANY = pl.BlockSpec(memory_space=pl.ANY)
HBM = pl.BlockSpec(memory_space=pltpu.HBM)


def shards(n, token_cond, atom_feat, atom_counts, w_token, w_query, w_key, w_value, w_out, w_back):
    tok, ct = token_cond.shape
    atom_rows, width = atom_feat.shape
    crow = tok // LANES
    counts = atom_counts.reshape(crow, LANES)
    nrow = 3 * crow + 4
    trows = 3 * tok + 3 * LANES
    tiles = atom_rows // LANES
    S = jax.ShapeDtypeStruct
    V = pltpu.VMEM
    DMA = pltpu.SemaphoreType.DMA
    prows = -(-(8 + crow * n + nrow) // 8) * 8
    group = 8
    I32 = jnp.int32
    hold = lambda x: pltpu.with_memory_space_constraint(x, pltpu.HBM)
    atoms, pooled = pl.pallas_call(
        functools.partial(whole, n, group),
        name="whole",
        out_shape=(S((atom_rows, width), BF16), S((tok, width), BF16)),
        in_specs=[HBM] * 8,
        out_specs=(VM, VM),
        scratch_shapes=[
            V((tok, ct), BF16), V((ct, width), BF16), V((atom_rows, width), BF16), V((width, 3 * width), BF16),
            V((width, width), BF16), V((trows, width), BF16), V((2 * HALO, width), BF16),
            V((n, crow, LANES), I32), V((prows, LANES), I32), V((prows, LANES), I32),
            V((nrow, LANES), I32), V((nrow, LANES), I32), V((8 + nrow, LANES), I32),
            pltpu.SMEM((8 + nrow, LANES), I32), V((tok, LANES), F32),
            V((atom_rows, width), BF16), V((atom_rows, width), BF16),
            V((atom_rows + 2 * HALO, width), BF16), V((atom_rows + 2 * HALO, width), BF16),
            V((atom_rows, width), BF16), V((atom_rows, 2 * LANES), BF16), V((2 * HALO, 2 * LANES), BF16),
            V(((tiles + 1) * 2 * LANES, width), F32),
            V((2, tok, width), BF16), V((2, tok, width), BF16),
            DMA((8 + crow,)), DMA((n - 1,)), DMA((n - 1,)), DMA((6,)), DMA((6,)), DMA((2, crow)), DMA((2, crow)),
        ],
        compiler_params=pltpu.CompilerParams(collective_id=0, has_side_effects=True, vmem_limit_bytes=24 << 20),
    )(*[hold(x) for x in (token_cond, w_token, atom_feat, counts, w_query, w_key, w_value, w_out)])
    token_out, atom_out = pl.pallas_call(
        finish,
        name="finish",
        out_shape=(S((tok, ct), BF16), S((atom_rows, width), BF16)),
        in_specs=[VM, VM, VM, VM],
        out_specs=(ANY, ANY),
        scratch_shapes=[V((tok, ct), BF16), DMA((1 + crow,))],
        compiler_params=pltpu.CompilerParams(vmem_limit_bytes=8 << 20),
    )(atoms, pooled, token_cond, w_back)
    return (token_out, atom_out)


def solution(mesh):
    both = P(("batch", "seq"), None)
    in_specs = (both, both, P(("batch", "seq")), P(), P(), P(), P(), P(), P())
    return jax.shard_map(
        functools.partial(shards, mesh.shape["seq"]), mesh=mesh, in_specs=in_specs, out_specs=(both, both),
        check_vma=False)
```

```python
import functools
import math

import jax
import jax.numpy as jnp
from jax import lax
from jax.experimental import pallas as pl
from jax.experimental.pallas import tpu as pltpu
from jax.sharding import PartitionSpec as P

HEADS = 4
QBLOCK = 32
KEYS = 128
HALO = 48
LANES = 128
MOST = 24
MESH = pl.DeviceIdType.MESH
F32 = jnp.float32
BF16 = jnp.bfloat16


def dot(a, b, dims=((1,), (0,))):
    return lax.dot_general(a, b, (dims, ((), ())), preferred_element_type=F32)


def greet(n, me):
    barrier = pltpu.get_barrier_semaphore()
    for d in range(1, n):
        pl.semaphore_signal(barrier, inc=1, device_id={"seq": lax.rem(me + d, n)}, device_id_type=MESH)
    return lambda: pl.semaphore_wait(barrier, n - 1)


def whole(n, group, cond_h, wtok_h, feat_h, counts_h, wq_h, wk_h, wv_h, wout_h, obuf, pooled_ref,
          cond, wtok, feat, wqkv, wout, table, halo, cnt, padded, ends_all, ends_v, starts_v, wins_v, wins, cols,
          xs, qs, ks, vs, att, mem, hmem, run, sbuf, got, lsem, csend, crecv, send_sem, recv_sem, ssend, srecv):
    me = lax.axis_index("seq")
    tok = cond.shape[0]
    atom_rows, width = feat.shape
    crow = tok // LANES
    head = width // HEADS
    nrow = ends_v.shape[0]
    scale = math.log2(math.e) / math.sqrt(head)
    step = group * LANES
    tiles = atom_rows // LANES
    groups = atom_rows // step
    right, left = lax.rem(me + 1, n), lax.rem(me + n - 1, n)
    right2, left2 = lax.rem(me + 2, n), lax.rem(me + n - 2, n)

    odd = lax.rem(me, 2)
    has_left, has_right = me > 0, me < n - 1

    def blank(at):
        table[pl.ds(at, tok), :] = jnp.zeros((tok, width), BF16)

    pl.when(me == 0)(lambda: blank(LANES))
    pl.when(me == n - 1)(lambda: blank(LANES + 2 * tok))
    arrive = greet(n, me)
    loads = [pltpu.make_async_copy(counts_h, cnt.at[me], lsem.at[0]),
             pltpu.make_async_copy(wtok_h, wtok, lsem.at[1])]
    loads += [pltpu.make_async_copy(cond_h.at[pl.ds(r * LANES, LANES)], cond.at[pl.ds(r * LANES, LANES)],
                                    lsem.at[8 + r]) for r in range(crow)]
    loads.append(pltpu.make_async_copy(feat_h, feat, lsem.at[2]))
    loads += [pltpu.make_async_copy(w, wqkv.at[:, pl.ds(i * width, width)], lsem.at[3 + i])
              for i, w in enumerate((wq_h, wk_h, wv_h))]
    loads.append(pltpu.make_async_copy(wout_h, wout, lsem.at[6]))
    for c in loads:
        c.start()

    base = LANES + tok
    table[pl.ds(0, LANES - HALO), :] = jnp.zeros((LANES - HALO, width), BF16)
    table[pl.ds(LANES + 3 * tok + HALO, 2 * LANES - HALO), :] = jnp.zeros((2 * LANES - HALO, width), BF16)
    run[pl.ds(0, 2 * LANES), :] = jnp.zeros((2 * LANES, width), F32)
    padded[...] = jnp.zeros_like(padded)
    loads[1].wait()
    for r in range(crow):
        loads[2 + r].wait()
        table[pl.ds(base + r * LANES, LANES), :] = dot(cond[pl.ds(r * LANES, LANES), :], wtok[...]).astype(BF16)
    loads[0].wait()
    loads[2 + crow].wait()
    arrive()

    ccopies = [pltpu.make_async_remote_copy(
        src_ref=cnt.at[me], dst_ref=cnt.at[me], send_sem=csend.at[d - 1], recv_sem=crecv.at[d - 1],
        device_id={"seq": lax.rem(me + d, n)}, device_id_type=MESH) for d in range(1, n)]

    def remote(i, src, dst, dev):
        return pltpu.make_async_remote_copy(
            src_ref=src, dst_ref=dst, send_sem=send_sem.at[i], recv_sem=recv_sem.at[i],
            device_id={"seq": dev}, device_id_type=MESH)

    copies = [
        remote(0, feat.at[pl.ds(atom_rows - HALO, HALO)], halo.at[pl.ds(0, HALO)], right),
        remote(1, feat.at[pl.ds(0, HALO)], halo.at[pl.ds(HALO, HALO)], left),
        remote(2, table.at[pl.ds(base + tok - HALO, HALO)], table.at[pl.ds(LANES - HALO, HALO)], right2),
        remote(3, table.at[pl.ds(base, HALO)], table.at[pl.ds(LANES + 3 * tok, HALO)], left2),
    ]
    for c in ccopies + copies:
        c.start()
    to_right = remote(4, table.at[pl.ds(base, tok)], table.at[pl.ds(LANES, tok)], right)
    to_left = remote(5, table.at[pl.ds(base, tok)], table.at[pl.ds(LANES + 2 * tok, tok)], left)
    pl.when((odd == 1) & has_right)(to_right.start)
    pl.when(has_left)(to_left.start)
    pl.when((odd == 0) & has_right)(to_right.start)

    def column(r):
        return jnp.transpose(jnp.broadcast_to(cnt[me, pl.ds(r, 1), :].astype(F32), (LANES, LANES)))

    for r in range(crow):
        cols[pl.ds(r * LANES, LANES), :] = column(r)
    for c in ccopies:
        c.wait()
    rows = padded.shape[0]
    for j in range(n):
        padded[pl.ds(8 + crow * j, crow), :] = cnt[j]
    counts = padded[...].astype(F32).astype(BF16)
    tri = (lax.broadcasted_iota(jnp.int32, (LANES, LANES), 0)
           <= lax.broadcasted_iota(jnp.int32, (LANES, LANES), 1)).astype(F32).astype(BF16)
    before = (lax.broadcasted_iota(jnp.int32, (rows, rows), 1)
              < lax.broadcasted_iota(jnp.int32, (rows, rows), 0)).astype(F32).astype(BF16)
    inner = dot(counts, tri)
    outer = jnp.sum(dot(before, counts), axis=1, keepdims=True)
    ends_all[...] = (inner + outer).astype(jnp.int32)
    near = pl.ds(8 - 1 - crow + crow * me, nrow)
    ends = ends_all[near, :] - me * atom_rows
    ends_v[...] = ends
    starts_v[...] = ends - padded[near, :]
    sizes = jnp.sum(padded[...], axis=1, keepdims=True)
    start = 8 - 1 - crow + crow * me
    past = lax.broadcasted_iota(jnp.int32, (rows, 1), 0) < start
    mark = jnp.sum(jnp.where(past, sizes, 0), axis=0, keepdims=True) - me * atom_rows
    near_sizes = jnp.sum(padded[near, :], axis=1, keepdims=True)
    first = jnp.where(lax.broadcasted_iota(jnp.int32, (8, LANES), 0) == 0,
                      lax.broadcasted_iota(jnp.int32, (8, LANES), 1) * LANES, -HALO)
    w = jnp.zeros_like(first)
    for r in range(nrow - 1):
        mark = mark + near_sizes[r:r + 1, :]
        w += jnp.where(mark <= first, 1, 0)
    w = jnp.minimum(w, nrow - 3)
    wins_v[pl.ds(0, 8), :] = w
    held = lax.broadcasted_iota(jnp.int32, (1, LANES), 1) < tiles
    w0 = jnp.where(held, w[0:1, :], nrow)
    block = lax.broadcasted_iota(jnp.int32, (nrow, LANES), 0)
    seen = jnp.sum(jnp.where(w0 <= block, 1, 0), axis=1, keepdims=True)
    last = w[0:1, tiles - 1:tiles]
    wins_v[pl.ds(8, nrow), :] = jnp.where(
        block <= last, seen * 2, jnp.where(block == last + 1, 2 * tiles + 1, 0))
    down = pltpu.make_async_copy(wins_v, wins, lsem.at[7])
    down.start()
    down.wait()

    def each(f):
        def body(g, c):
            f(g)
            return c
        return body

    def members(w, first, r):
        ids = first + lax.broadcasted_iota(jnp.int32, (r, LANES), 0)
        parts = []
        for s in range(2):
            lo = starts_v[pl.ds(w + s, 1), :]
            hi = ends_v[pl.ds(w + s, 1), :]
            parts.append(jnp.where((ids >= lo) & (ids < hi), F32(1), F32(0)).astype(BF16))
        return jnp.concatenate(parts, axis=1)

    def gather(w, member, f):
        picked = dot(member, table[pl.ds(w * LANES, 2 * LANES), :])
        return (f.astype(F32) + picked).astype(BF16)

    def build(i):
        a = pl.multiple_of(i * LANES, LANES)
        mem[pl.ds(a, LANES), :] = members(wins[0, i], a, LANES)

    lax.fori_loop(0, tiles, each(build), 0)
    outside = ((-HALO, 0, wins[1, 0]), (atom_rows, atom_rows + HALO, wins[0, tiles]))
    for i, (start, _, w) in enumerate(outside):
        hmem[pl.ds(i * HALO, HALO), :] = members(w, jnp.int32(start), HALO)
    for c in loads[3 + crow:]:
        c.wait()
    for c in copies:
        c.wait()
    pl.when(has_left)(to_right.wait_recv)
    pl.when(has_right)(to_left.wait_recv)

    def keyval(at, qkv, r):
        ks[pl.ds(at, r), :] = qkv[:, width:2 * width].astype(BF16)
        vs[pl.ds(at, r), :] = qkv[:, 2 * width:].astype(BF16)

    for i, (_, at, w) in enumerate(outside):
        x = gather(w, hmem[pl.ds(i * HALO, HALO), :], halo[pl.ds(i * HALO, HALO), :])
        keyval(at, dot(x, wqkv[...]), HALO)

    lane = lax.broadcasted_iota(jnp.int32, (1, width), 1)
    hmask = [((lane >= h * head) & (lane < (h + 1) * head)) for h in range(HEADS)]
    hmul = [jnp.where(m, F32(1), F32(0)).astype(BF16) for m in hmask]
    ones = jnp.ones((KEYS, width), BF16)
    total = atom_rows * n
    klane = lax.broadcasted_iota(jnp.int32, (1, KEYS), 1)
    per = LANES // QBLOCK
    unit = group // 4

    def pick(o):
        r = o[(HEADS - 1) * QBLOCK:]
        for h in range(HEADS - 2, -1, -1):
            r = jnp.where(hmask[h], o[h * QBLOCK:(h + 1) * QBLOCK], r)
        return r

    def gathers(g):
        made = []
        for u in range(group):
            a = pl.multiple_of(g * step + u * LANES, LANES)
            made.append((a, gather(wins[0, g * group + u], mem[pl.ds(a, LANES), :], feat[pl.ds(a, LANES), :])))
        return made

    def project(made):
        qkvs = [dot(x, wqkv[...]) for _, x in made]
        for (a, x), qkv in zip(made, qkvs):
            xs[pl.ds(a, LANES), :] = x
            qs[pl.ds(a, LANES), :] = qkv[:, :width].astype(BF16)
            keyval(pl.multiple_of(a + HALO, 16), qkv, LANES)

    def scored(g, js):
        scores = []
        for j in js:
            at = pl.multiple_of(g * step + j * QBLOCK, QBLOCK)
            q = qs[pl.ds(at, QBLOCK), :]
            qb = jnp.concatenate([q * m for m in hmul], axis=0)
            s = dot(qb, ks[pl.ds(at, KEYS), :], ((1,), (1,)))
            pos = me * atom_rows + at - HALO + klane
            scores.append(jnp.where((pos >= 0) & (pos < total), s, F32(-1e30)))
        return scores

    def soft(scores):
        probs = []
        for s in scores:
            m = jnp.max(s, axis=1, keepdims=True)
            probs.append(jnp.exp2((s - m) * F32(scale)).astype(BF16))
        return probs

    def attend(g, js, probs):
        raw = []
        for j, p in zip(js, probs):
            at = pl.multiple_of(g * step + j * QBLOCK, QBLOCK)
            raw.append(dot(p, jnp.concatenate([vs[pl.ds(at, KEYS), :], ones], axis=1)))
        return [(pick(o[:, :width]) / pick(o[:, width:])).astype(BF16) for o in raw]

    def residual(tile):
        at = pl.ds(pl.multiple_of(tile * LANES, LANES), unit * LANES)
        y = (xs[at, :].astype(F32) + dot(att[at, :], wout[...])).astype(BF16)
        obuf[at, :] = y
        return y

    def pooled(tile, y):
        parts = [dot(mem[pl.ds(pl.multiple_of((tile + u) * LANES, LANES), LANES), :],
                     y[u * LANES:(u + 1) * LANES], ((0,), (0,))) for u in range(unit)]
        at = pl.multiple_of(2 * LANES * tile, 2 * LANES)
        acc = run[pl.ds(at, 2 * LANES), :]
        for u, part in enumerate(parts):
            i = tile + u
            same = wins[0, i] == wins[0, jnp.maximum(i - 1, 0)]
            low = jnp.where(same, acc[:LANES], acc[LANES:])
            high = jnp.where(same, acc[LANES:], F32(0))
            acc = part + jnp.concatenate([low, high], axis=0)
            run[pl.ds(pl.multiple_of(at + (u + 1) * 2 * LANES, 2 * LANES), 2 * LANES), :] = acc

    def sums(b):
        return run[pl.ds(wins[8 + b, 0] * LANES, LANES), :]

    def side(i, dev, r):
        at = pl.ds(r * LANES, LANES)
        return pltpu.make_async_remote_copy(
            src_ref=sbuf.at[i, at], dst_ref=got.at[i, at], send_sem=ssend.at[i, r], recv_sem=srecv.at[i, r],
            device_id={"seq": dev}, device_id_type=MESH)

    def share(i, dev, r):
        sbuf[i, pl.ds(r * LANES, LANES), :] = sums(1 + 2 * crow * i + r).astype(BF16)
        side(i, dev, r).start()

    ahead = 1
    ready = min((tiles - group // 2) // MOST, crow)


    def advance(g, more):
        start = g * group
        q = [range(k * unit * per, (k + 1) * unit * per) for k in range(4)]

        def keep(k, p):
            at = pl.ds(pl.multiple_of((start + k * unit) * LANES, LANES), unit * LANES)
            att[at, :] = jnp.concatenate(attend(g, q[k], p), axis=0)

        past = jnp.maximum(start - unit, 0)
        s0 = scored(g, q[0])
        y = residual(past)
        made = gathers(g + ahead) if more else None
        s1 = scored(g, q[1])
        p0 = soft(s0)
        if more:
            project(made)
        keep(0, p0)
        s2 = scored(g, q[2])
        p1 = soft(s1)
        pooled(past, y)
        y = residual(start)
        keep(1, p1)
        s3 = scored(g, q[3])
        p2 = soft(s2)
        pooled(start, y)
        y = residual(start + unit)
        keep(2, p2)
        p3 = soft(s3)
        pooled(start + unit, y)
        if not more:
            for r in range(ready):
                pl.when(has_left)(functools.partial(share, 0, left, r))
        y = residual(start + 2 * unit)
        keep(3, p3)
        pooled(start + 2 * unit, y)

    lax.fori_loop(0, ahead, each(lambda g: project(gathers(g))), 0)
    lax.fori_loop(0, groups - ahead, each(lambda g: advance(g, True)), 0)
    lax.fori_loop(groups - ahead, groups, each(lambda g: advance(g, False)), 0)
    y = residual(tiles - unit)
    pooled(tiles - unit, y)

    for r in range(crow):
        pl.when((odd == 1) & has_right)(functools.partial(share, 1, right, r))
    for r in range(ready, crow):
        pl.when(has_left)(functools.partial(share, 0, left, r))
    for r in range(crow):
        pl.when((odd == 0) & has_right)(functools.partial(share, 1, right, r))
    for r in range(crow):
        at = pl.ds(r * LANES, LANES)
        pl.when(has_left)(side(1, right, r).wait_recv)
        pl.when(has_right)(side(0, left, r).wait_recv)
        s = (sums(1 + crow + r) + jnp.where(has_right, got[0, at, :].astype(F32), 0)
             + jnp.where(has_left, got[1, at, :].astype(F32), 0))
        pooled_ref[at, :] = (s / cols[at, :]).astype(BF16)
    pl.when(has_right)(to_right.wait_send)
    pl.when(has_left)(to_left.wait_send)
    for r in range(crow):
        pl.when(has_right)(side(1, right, r).wait_send)
        pl.when(has_left)(side(0, left, r).wait_send)


def finish(atoms_ref, pooled_ref, cond_ref, wback_ref, token_ref, out_ref, tbuf, sem):
    tok = cond_ref.shape[0]
    out = pltpu.make_async_copy(atoms_ref, out_ref, sem.at[0])
    out.start()
    copies = []
    for r in range(tok // LANES):
        at = pl.ds(r * LANES, LANES)
        tbuf[at, :] = (cond_ref[at, :].astype(F32) + dot(pooled_ref[at, :], wback_ref[...])).astype(BF16)
        c = pltpu.make_async_copy(tbuf.at[at], token_ref.at[at], sem.at[1 + r])
        c.start()
        copies.append(c)
    for c in copies:
        c.wait()
    out.wait()


VM = pl.BlockSpec(memory_space=pltpu.VMEM)
ANY = pl.BlockSpec(memory_space=pl.ANY)
HBM = pl.BlockSpec(memory_space=pltpu.HBM)


def shards(n, token_cond, atom_feat, atom_counts, w_token, w_query, w_key, w_value, w_out, w_back):
    tok, ct = token_cond.shape
    atom_rows, width = atom_feat.shape
    crow = tok // LANES
    counts = atom_counts.reshape(crow, LANES)
    nrow = 3 * crow + 4
    trows = 3 * tok + 3 * LANES
    tiles = atom_rows // LANES
    S = jax.ShapeDtypeStruct
    V = pltpu.VMEM
    DMA = pltpu.SemaphoreType.DMA
    prows = -(-(8 + crow * n + nrow) // 8) * 8
    group = 16
    I32 = jnp.int32
    hold = lambda x: pltpu.with_memory_space_constraint(x, pltpu.HBM)
    atoms, pooled = pl.pallas_call(
        functools.partial(whole, n, group),
        name="whole",
        out_shape=(S((atom_rows, width), BF16), S((tok, width), BF16)),
        in_specs=[HBM] * 8,
        out_specs=(VM, VM),
        scratch_shapes=[
            V((tok, ct), BF16), V((ct, width), BF16), V((atom_rows, width), BF16), V((width, 3 * width), BF16),
            V((width, width), BF16), V((trows, width), BF16), V((2 * HALO, width), BF16),
            V((n, crow, LANES), I32), V((prows, LANES), I32), V((prows, LANES), I32),
            V((nrow, LANES), I32), V((nrow, LANES), I32), V((8 + nrow, LANES), I32),
            pltpu.SMEM((8 + nrow, LANES), I32), V((tok, LANES), F32),
            V((atom_rows, width), BF16), V((atom_rows, width), BF16),
            V((atom_rows + 2 * HALO, width), BF16), V((atom_rows + 2 * HALO, width), BF16),
            V((atom_rows, width), BF16), V((atom_rows, 2 * LANES), BF16), V((2 * HALO, 2 * LANES), BF16),
            V(((tiles + 1) * 2 * LANES, width), F32),
            V((2, tok, width), BF16), V((2, tok, width), BF16),
            DMA((8 + crow,)), DMA((n - 1,)), DMA((n - 1,)), DMA((6,)), DMA((6,)), DMA((2, crow)), DMA((2, crow)),
        ],
        compiler_params=pltpu.CompilerParams(collective_id=0, has_side_effects=True, vmem_limit_bytes=24 << 20),
    )(*[hold(x) for x in (token_cond, w_token, atom_feat, counts, w_query, w_key, w_value, w_out)])
    token_out, atom_out = pl.pallas_call(
        finish,
        name="finish",
        out_shape=(S((tok, ct), BF16), S((atom_rows, width), BF16)),
        in_specs=[VM, VM, VM, VM],
        out_specs=(ANY, ANY),
        scratch_shapes=[V((tok, ct), BF16), DMA((1 + crow,))],
        compiler_params=pltpu.CompilerParams(vmem_limit_bytes=8 << 20),
    )(atoms, pooled, token_cond, w_back)
    return (token_out, atom_out)


def solution(mesh):
    both = P(("batch", "seq"), None)
    in_specs = (both, both, P(("batch", "seq")), P(), P(), P(), P(), P(), P())
    return jax.shard_map(
        functools.partial(shards, mesh.shape["seq"]), mesh=mesh, in_specs=in_specs, out_specs=(both, both),
        check_vma=False)
```
